32 devices in a mesh: dp: 8 (over y, x, core), tp: 4 (over z).
Axes of the slice: x: 2, y: 2, z: 4, core: 2. Of those that a mesh axis runs over, the one named last changes fastest.
Arguments:
- x_tokens: bfloat16 [8192, 8192], P(('dp', 'tp')), may hold values from -6 to 6
- segment_ids: int32 [8, 1024], P('dp'), may hold values from 0 to 3, never falling along the last dimension, each value on 1 to 512 neighbouring positions
- attended_grad: bfloat16 [8192, 4096], P('dp', 'tp'), may hold values from -6 to 6
- norm_gain: float32 [8192], replicated, may hold values from 0.1 to 1.9
- w_query: bfloat16 [8192, 4096], P(None, 'tp'), may hold values from -1 to 1
- w_key: bfloat16 [8192, 1024], P(None, 'tp'), may hold values from -4 to 4
- w_value: bfloat16 [8192, 1024], P(None, 'tp'), may hold values from -0.0625 to 0.0625
Outputs:
- attended: bfloat16 [8192, 4096], P('dp', 'tp')
- input_grad: bfloat16 [8192, 8192], P(('dp', 'tp'))
- gain_grad: float32 [8192], replicated
- grad_query: float32 [8192, 4096], P('dp', 'tp')
- grad_key: float32 [8192, 1024], P('dp', 'tp')
- grad_value: float32 [8192, 1024], P('dp', 'tp')
The draws below stay inside these ranges and needn't reach their ends.
Inputs may be any that keep to these rules, and one draw needn't show every extreme that they name: `segment_ids`: along each replica's row the numbers never fall; every number 0 to 3 covers one run of 1 to 512 positions.
All inputs are finite; a program needn't handle non-finite values.
Results may differ from the reference program's by a relative error of at most 0.028.
The reference program's roundings to bfloat16 on the way count: a program that leaves them out, or rounds other values in their place, can miss the bound.
Values may be sent and summed in bfloat16 or wider, within the bound.
No kernel may reach another device: no remote copies, remote signals or barrier semaphores. Data moves between devices by JAX's collectives and lax.ppermute only.
A program may use at most 256 MiB of HBM per device.

```python
import math
import jax
import jax.numpy as jnp
import numpy as np
from jax import lax

D = 8192
QH = 32
KVH = 8
HD = 128
SEQ = 1024
TOKENS = 8192
N_DP = 8
N_TP = 4


def query_matrix(key):
    raw = jax.random.normal(jax.random.fold_in(key, 11), (D, QH * HD), jnp.float32) / math.sqrt(D)
    return jnp.clip(raw, -1.0, 1.0)


def draw_w_query(key, part):
    return query_matrix(key).astype(jnp.bfloat16)


def draw_w_key(key, part):
    noise = jax.random.normal(jax.random.fold_in(key, 12), (D, KVH * HD), jnp.float32) / math.sqrt(D)
    return jnp.clip(noise, -4.0, 4.0).astype(jnp.bfloat16)


def spiked(result, key, source, target, shards_of, factor):
    owner, partner = [(jnp.arange(result.shape[dim]) // (result.shape[dim] // shards_of)).reshape([-1 if axis == dim else 1 for axis in range(result.ndim)]) for dim in (source, target)]
    chosen = jax.random.permutation(key, shards_of)[partner]
    strong = (owner == chosen) | (owner == (partner + shards_of // 2) % shards_of)
    return jnp.where(strong, factor * result, result)


def block_scale(stream_key, extent, pieces, smallest, top_value):
    gain, own = 1.0, jax.random.fold_in(stream_key, 6)
    for axis_at, blocks in pieces:
        heights = jnp.exp(jax.random.uniform(jax.random.fold_in(own, axis_at), (blocks,), jnp.float32, smallest / len(pieces), top_value / len(pieces)))
        gain = gain * jnp.repeat(heights, extent[axis_at] // blocks).reshape([-1 if axis == axis_at else 1 for axis in range(len(extent))])
    return gain


def profile(count, total, bound, skew):
    portions = [(1 << 20) // math.isqrt(grade ** skew) + 1 for grade in range(2, count + 1)]
    rest, counts = total - bound - (count - 1), [1] * (count - 1)
    while rest > 0:
        movable = [i for i in range(count - 1) if counts[i] < bound]
        whole, remaining = sum([portions[i] for i in movable]), rest
        for i in movable:
            addition = min(bound - counts[i], max(1, remaining * portions[i] // whole), rest)
            counts[i] = counts[i] + addition
            rest = rest - addition
    return np.array([bound] + counts)


def uneven_parts(stream_key, amount, total, limit, lean):
    if amount == 2:
        one = jax.random.randint(stream_key, (), max(1, total - limit), min(limit, total - 1) + 1)
        return jnp.stack([one, total - one])
    tallies = jnp.asarray(profile(amount, total, limit, lean), jnp.int32)
    pairs = (amount - 1) // 2
    source_of, receiver = tallies[1:1 + 2 * pairs:2], tallies[2:2 + 2 * pairs:2]
    room = jnp.minimum(source_of - 1, limit - receiver)
    moved = jax.random.randint(jax.random.fold_in(stream_key, 1), (pairs,), 0, 1 << 20) % (room + 1)
    tallies = tallies.at[1:1 + 2 * pairs:2].set(source_of - moved).at[2:2 + 2 * pairs:2].set(receiver + moved)
    return tallies[jax.random.permutation(jax.random.fold_in(stream_key, 2), amount)]


def gaussian(stream_key, extent, width, limit, shards=(), kind=jnp.bfloat16):
    loudness = block_scale(stream_key, extent, shards, -0.22, 0.18) if shards else 1.0
    entries = jax.random.normal(stream_key, extent, jnp.float32) * width * loudness
    return jnp.minimum(jnp.maximum(entries, -limit), limit).astype(kind)


def heavy_noise(key, shape, deviation, bound, shards, heavy, kind=jnp.bfloat16):
    drawn = deviation * jax.random.normal(key, shape, jnp.float32)
    if shards:
        drawn = drawn * block_scale(key, shape, shards, -0.22, 0.18)
    return jnp.clip(spiked(drawn, jax.random.fold_in(key, 3), *heavy), -bound, bound).astype(kind)


def setup_inputs(seed: int = 0) -> dict:
    keys = jax.random.split(jax.random.key(seed), 8)
    return {
        "x_tokens": heavy_noise(keys[0], (TOKENS, D), 1.0, 6.0, ((0, 32),), (0, 1, 32, 2.75)),
        "segment_ids": jax.vmap(lambda own: jnp.searchsorted(jnp.cumsum(uneven_parts(own, 4, SEQ, SEQ // 2, 1)), jnp.arange(SEQ), side="right"))(jax.random.split(keys[1], N_DP)).reshape((N_DP, SEQ)).astype(jnp.int32),
        "attended_grad": gaussian(keys[2], (TOKENS, QH * HD), 1.0, 6.0, ((0, 8), (1, 4))),
        "norm_gain": jnp.clip(1.0 + 0.18 * jax.random.normal(keys[3], (D,), jnp.float32), 0.1, 1.9),
        "w_query": draw_w_query(jax.random.fold_in(keys[7], 71), 0),
        "w_key": draw_w_key(jax.random.fold_in(keys[7], 71), 0),
        "w_value": gaussian(keys[6], (D, KVH * HD), D ** -0.5, 0.0625, ((1, 4),)),
    }


epsilon = 1e-05
rope_base = 500000.0

def rope_tables(segment_row):
    length = segment_row.shape[0]
    earlier = (segment_row[None, :] < segment_row[:, None]).astype(jnp.int32)
    offset = jnp.arange(length, dtype=jnp.int32) - lax.optimization_barrier(jnp.sum(earlier, axis=1)).astype(jnp.int32)
    half_dim = HD // 2
    inverse_freq = rope_base ** (-(jnp.arange(half_dim, dtype=jnp.float32) * 2.0 / HD))
    angle = offset.astype(jnp.float32)[:, None] * inverse_freq[None, :]
    return (jnp.cos(angle)[:, None, :], jnp.sin(angle)[:, None, :])

def attend_mask(segment_row):
    length = segment_row.shape[0]
    position = jnp.arange(length, dtype=jnp.int32)
    return (position[None, :] <= position[:, None]) & (segment_row[None, :] == segment_row[:, None])

def apply_rope(head_rows, cosine_table, sine_table, direction):
    half_dim = head_rows.shape[-1] // 2
    first_half = head_rows[..., :half_dim]
    second_half = head_rows[..., half_dim:]
    return jnp.concatenate([first_half * cosine_table - direction * second_half * sine_table, second_half * cosine_table + direction * first_half * sine_table], axis=-1)

def group_sum(left_parts, right_parts):
    lefts = jnp.concatenate([part.reshape(SEQ, N_TP, -1) for part in left_parts], axis=2).astype(jnp.float32)
    rights = jnp.concatenate([part.reshape(N_TP, -1, D) for part in right_parts], axis=1).astype(jnp.float32)
    partial_sums = jnp.einsum('sgc,gcd->gsd', lefts, rights)
    rounded = lax.optimization_barrier(partial_sums.astype(jnp.bfloat16))
    return lax.optimization_barrier(jnp.sum(rounded.astype(jnp.float32), axis=0))

def replica(x_rows, segment_row, grad_rows, norm_gain, w_query, w_key, w_value):
    group = QH // KVH
    score_scale = float(HD) ** (-0.5)
    as_float = x_rows.astype(jnp.float32)
    inverse = lax.rsqrt(lax.optimization_barrier(jnp.mean(as_float * as_float, axis=1, keepdims=True)) + epsilon)
    x_hat = as_float * inverse
    normed = (x_hat * norm_gain).astype(jnp.bfloat16)
    cosine_table, sine_table = rope_tables(segment_row)
    allowed = attend_mask(segment_row)
    query_f = jnp.dot(normed, w_query, preferred_element_type=jnp.float32).reshape(SEQ, QH, HD)
    queries = apply_rope(query_f, cosine_table, sine_table, 1.0).astype(jnp.bfloat16)
    key_f = jnp.dot(normed, w_key, preferred_element_type=jnp.float32).reshape(SEQ, KVH, HD)
    key_rows = apply_rope(key_f, cosine_table, sine_table, 1.0).astype(jnp.bfloat16)
    values_in = jnp.dot(normed, w_value, preferred_element_type=jnp.float32).astype(jnp.bfloat16).reshape(SEQ, KVH, HD)
    grouped = queries.reshape(SEQ, KVH, group, HD).astype(jnp.float32)
    scores = jnp.einsum('skgd,tkd->kgst', grouped, key_rows.astype(jnp.float32)) * score_scale
    scores = jnp.where(allowed[None, None], scores, -1e+30)
    highest = lax.optimization_barrier(jnp.max(scores, axis=3, keepdims=True))
    exponent = jnp.exp(scores - highest)
    probability = exponent / lax.optimization_barrier(jnp.sum(exponent, axis=3, keepdims=True))
    weights_b = probability.astype(jnp.bfloat16)
    attended = jnp.einsum('kgst,tkd->skgd', weights_b.astype(jnp.float32), values_in.astype(jnp.float32)).astype(jnp.bfloat16)
    attended_flat = attended.reshape(SEQ, QH * HD)
    out_grouped = grad_rows.reshape(SEQ, KVH, group, HD).astype(jnp.float32)
    row_delta = lax.optimization_barrier(jnp.sum(out_grouped * attended.astype(jnp.float32), axis=3))
    value_d = jnp.einsum('kgst,skgd->tkd', weights_b.astype(jnp.float32), out_grouped).astype(jnp.bfloat16)
    prob_d = jnp.einsum('skgd,tkd->kgst', out_grouped, values_in.astype(jnp.float32))
    score_d = (probability * (prob_d - jnp.transpose(row_delta, (1, 2, 0))[..., None]) * score_scale).astype(jnp.bfloat16)
    query_rot = jnp.einsum('kgst,tkd->skgd', score_d.astype(jnp.float32), key_rows.astype(jnp.float32)).reshape(SEQ, QH, HD)
    key_rot = jnp.einsum('kgst,skgd->tkd', score_d.astype(jnp.float32), grouped)
    query_d = apply_rope(query_rot, cosine_table, sine_table, -1.0).astype(jnp.bfloat16).reshape(SEQ, QH * HD)
    key_d = apply_rope(key_rot, cosine_table, sine_table, -1.0).astype(jnp.bfloat16).reshape(SEQ, KVH * HD)
    value_flat = value_d.reshape(SEQ, KVH * HD)
    normed_d = group_sum([query_d, key_d, value_flat], [w_query.T, w_key.T, w_value.T])
    scaled_d = normed_d * norm_gain
    input_grad = (inverse * (scaled_d - x_hat * lax.optimization_barrier(jnp.mean(scaled_d * x_hat, axis=1, keepdims=True)))).astype(jnp.bfloat16)
    gain_term = lax.optimization_barrier(jnp.sum(normed_d * x_hat, axis=0))
    grads = (jnp.dot(normed.T, query_d, preferred_element_type=jnp.float32).astype(jnp.bfloat16), jnp.dot(normed.T, key_d, preferred_element_type=jnp.float32).astype(jnp.bfloat16), jnp.dot(normed.T, value_flat, preferred_element_type=jnp.float32).astype(jnp.bfloat16))
    return (attended_flat, input_grad, gain_term, grads)

def reference(x_tokens, segment_ids, attended_grad, norm_gain, w_query, w_key, w_value):
    x_blocks = x_tokens.reshape(N_DP, SEQ, D)
    grad_blocks = attended_grad.reshape(N_DP, SEQ, QH * HD)
    initial = (jnp.zeros((D, QH * HD), jnp.float32), jnp.zeros((D, KVH * HD), jnp.float32), jnp.zeros((D, KVH * HD), jnp.float32), jnp.zeros((D,), jnp.float32))

    def replica_step(running, inputs):
        x_rows, segment_row, grad_rows = inputs
        attended_flat, input_grad, gain_term, grads = replica(x_rows, segment_row, grad_rows, norm_gain, w_query, w_key, w_value)
        grads = lax.optimization_barrier(grads)
        summed = tuple((total + grad.astype(jnp.float32) for total, grad in zip(running[:3], grads)))
        return (summed + (running[3] + gain_term,), (attended_flat, input_grad))
    totals, (outputs, input_grads) = lax.scan(replica_step, initial, (x_blocks, segment_ids, grad_blocks))
    return (outputs.reshape(N_DP * SEQ, QH * HD), input_grads.reshape(N_DP * SEQ, D), totals[3], totals[0], totals[1], totals[2])
```

```python
import functools

import jax
import jax.numpy as jnp
from jax import lax
from jax.experimental import pallas as pl
from jax.experimental.pallas import tpu as pltpu
from jax.sharding import PartitionSpec as P


HD = 128


epsilon = 1e-05
rope_base = 500000.0


def rope_tables(segment_row, head_dim):
    length = segment_row.shape[0]
    earlier = (segment_row[None, :] < segment_row[:, None]).astype(jnp.int32)
    offset = jnp.arange(length, dtype=jnp.int32) - jnp.sum(earlier, axis=1)
    half_dim = head_dim // 2
    inverse_freq = rope_base ** (-(jnp.arange(half_dim, dtype=jnp.float32) * 2.0 / head_dim))
    angle = offset.astype(jnp.float32)[:, None] * inverse_freq[None, :]
    return (jnp.cos(angle)[:, None, :], jnp.sin(angle)[:, None, :])


def apply_rope(head_rows, cosine_table, sine_table, direction):
    half_dim = head_rows.shape[-1] // 2
    first_half = head_rows[..., :half_dim]
    second_half = head_rows[..., half_dim:]
    return jnp.concatenate(
        [
            first_half * cosine_table - direction * second_half * sine_table,
            second_half * cosine_table + direction * first_half * sine_table,
        ],
        axis=-1,
    )


def contract_first(left, right):
    return lax.dot_general(
        left, right, (((0,), (0,)), ((), ())), preferred_element_type=jnp.float32
    )


def contract_last(left, right):
    return lax.dot_general(
        left, right, (((1,), (1,)), ((), ())), preferred_element_type=jnp.float32
    )


def turn_back(rows_f, cosine, sine):
    return rows_f * cosine + pltpu.roll(rows_f, rows_f.shape[1] // 2, 1) * sine


def attention_kernel(
    block_rows, query_ref, key_ref, value_ref, grad_ref, segment_column, segment_line,
    cosine_ref, sine_ref, attended_ref, query_d_ref, key_d_ref, value_d_ref, key_sum, value_sum,
):
    member = pl.program_id(1)
    seq_len, head_dim = query_ref.shape
    score_scale = float(head_dim) ** (-0.5)

    @pl.when(member == 0)
    def _():
        key_sum[...] = jnp.zeros_like(key_sum)
        value_sum[...] = jnp.zeros_like(value_sum)

    for first in range(0, seq_len, block_rows):
        last = first + block_rows
        query = query_ref[first:last, :]
        grad = grad_ref[first:last, :]
        keys = key_ref[:last, :]
        values = value_ref[:last, :]
        scores = contract_last(query, keys) * score_scale
        row = lax.broadcasted_iota(jnp.int32, scores.shape, 0) + first
        column = lax.broadcasted_iota(jnp.int32, scores.shape, 1)
        same = segment_column[first:last, :] == segment_line[:, :last]
        scores = jnp.where((column <= row) & same, scores, -1e30)
        exponent = jnp.exp(scores - jnp.max(scores, axis=1, keepdims=True))
        probability = exponent * (1.0 / jnp.sum(exponent, axis=1, keepdims=True))
        weights_b = probability.astype(jnp.bfloat16)
        attended = jnp.dot(weights_b, values, preferred_element_type=jnp.float32)
        attended = attended.astype(jnp.bfloat16)
        attended_ref[first:last, :] = attended
        row_delta = jnp.sum(
            grad.astype(jnp.float32) * attended.astype(jnp.float32), axis=1, keepdims=True
        )
        value_sum[:last, :] += contract_first(weights_b, grad)
        prob_d = contract_last(grad, values)
        score_d = (probability * (prob_d - row_delta) * score_scale).astype(jnp.bfloat16)
        query_rot = jnp.dot(score_d, keys, preferred_element_type=jnp.float32)
        query_d_ref[first:last, :] = turn_back(
            query_rot, cosine_ref[first:last, :], sine_ref[first:last, :]
        ).astype(jnp.bfloat16)
        key_sum[:last, :] += contract_first(score_d, query)

    @pl.when(member == pl.num_programs(1) - 1)
    def _():
        key_d_ref[...] = turn_back(key_sum[...], cosine_ref[...], sine_ref[...]).astype(
            jnp.bfloat16
        )
        value_d_ref[...] = value_sum[...].astype(jnp.bfloat16)


def attend(projected, attended_grad, segment_row, cosine_table, sine_table, q_heads, kv_heads):
    seq_len, head_dim = projected.shape[0], HD
    group = q_heads // kv_heads
    block_rows = 256 if seq_len % 256 == 0 else seq_len
    cosine = jnp.concatenate([cosine_table[:, 0], cosine_table[:, 0]], axis=1)
    sine = jnp.concatenate([sine_table[:, 0], -sine_table[:, 0]], axis=1)

    def head(index_of):
        return pl.BlockSpec((seq_len, head_dim), lambda k, m: (0, index_of(k, m)))

    def whole(shape):
        return pl.BlockSpec(shape, lambda k, m: (0, 0))

    of_query = head(lambda k, m: k * group + m)
    of_key = head(lambda k, m: k)
    pairs = q_heads * seq_len * seq_len
    return pl.pallas_call(
        functools.partial(attention_kernel, block_rows),
        grid=(kv_heads, group),
        in_specs=[
            of_query,
            head(lambda k, m: q_heads + k),
            head(lambda k, m: q_heads + kv_heads + k),
            of_query,
            whole((seq_len, 1)),
            whole((1, seq_len)),
            whole((seq_len, head_dim)),
            whole((seq_len, head_dim)),
        ],
        out_specs=[of_query, of_query, of_key, of_key],
        out_shape=[
            jax.ShapeDtypeStruct((seq_len, heads * head_dim), jnp.bfloat16)
            for heads in (q_heads, q_heads, kv_heads, kv_heads)
        ],
        scratch_shapes=[pltpu.VMEM((seq_len, head_dim), jnp.float32)] * 2,
        cost_estimate=pl.CostEstimate(
            flops=8 * pairs * head_dim, bytes_accessed=10 * projected.size, transcendentals=pairs
        ),
    )(
        projected, projected, projected, attended_grad, segment_row[:, None],
        segment_row[None, :], cosine, sine,
    )


def total_over(value, axis):
    size = lax.axis_size(axis)
    if size & (size - 1):
        return lax.psum(value, axis)
    apart = 1
    while apart < size:
        value = value + lax.ppermute(value, axis, [(i, i ^ apart) for i in range(size)])
        apart *= 2
    return value


def right_pairs(low, high):
    return [(i, i + 1) for i in range(low, high)]


def left_pairs(low, high):
    return [(i, i - 1) for i in range(low, high)]


def split_rows(block):
    half = block.shape[0] // 2
    return [block[:half], block[half:]]


def send(pieces, pairs):
    sent = []
    for piece in pieces:
        sent.append(lax.ppermute(piece, "tp", pairs))
    return sent


def end_weights(w_query, w_key, w_value, tp):
    share = w_query.shape[0] // lax.axis_size("dp")
    first = lax.axis_index("dp") * share
    cut = [lax.dynamic_slice_in_dim(w, first, share, 0) for w in (w_query, w_key, w_value)]
    cut = lax.optimization_barrier(jnp.concatenate(cut, axis=1))
    [passed] = send([cut], [(0, 1), (tp - 1, tp - 2)])
    return passed


def shared(passed, after):
    passed, _ = lax.optimization_barrier((passed, after))
    return lax.all_gather(passed, "dp", axis=0, tiled=True)


def line_gather(own, tp, me, steps):
    found = [(own, me)]
    rightward = leftward = own
    for step in range(1, steps):
        rightward = send(rightward, right_pairs(step - 1, tp - 1))
        leftward = send(leftward, left_pairs(1, tp - step + 1))
        if 2 * step >= tp:
            left_over = leftward
            place = jnp.where(me >= step, me - step, me + step)
            if 2 * step > tp:
                empty = (me < step) & (me + step >= tp)
                left_over = [jnp.where(empty, o, l) for o, l in zip(own, leftward)]
                place = jnp.where(empty, me, place)
            chosen = [jnp.where(me >= step, r, l) for r, l in zip(rightward, left_over)]
            found.append((chosen, place))
        else:
            found.append((rightward, (me - step + tp) % tp))
            found.append((leftward, (me + step) % tp))
    return found


def line_scatter(columns_d, weights, far_weights, tp, me, rows):
    def rows_of(place):
        return lax.dynamic_slice(columns_d, (place * rows, 0), (rows, columns_d.shape[1]))

    def part(place):
        return contract_last(rows_of(place), weights)

    def ahead_of(step):
        return jnp.where(me + step < tp, me + step, (me - step + tp) % tp)

    from_left = from_right = None
    first_sent = columns_d
    start = tp - 1
    extra = None
    if far_weights is not None:
        far = lax.optimization_barrier(rows_of(tp - 1 - me))
        far = lax.ppermute(far, "tp", [(0, 1), (tp - 1, tp - 2)])
        start = tp - 2
        own_first = lax.optimization_barrier(part(ahead_of(start)))
        extra = contract_last(far, far_weights)
    for step in range(start, 0, -1):
        if 2 * step >= tp:
            ahead = own_first if extra is not None else part(ahead_of(step))
            if extra is not None:
                ahead, extra = ahead + extra, None
            if from_left is not None:
                ahead = ahead + from_left.astype(jnp.float32) + from_right.astype(jnp.float32)
            rightward = leftward = lax.optimization_barrier(ahead.astype(jnp.bfloat16))
        else:
            rightward = lax.optimization_barrier(part((me + step) % tp))
            leftward = lax.optimization_barrier(part((me - step + tp) % tp))
            if from_left is not None:
                rightward = rightward + from_left.astype(jnp.float32)
                leftward = leftward + from_right.astype(jnp.float32)
            rightward = rightward.astype(jnp.bfloat16)
            leftward = leftward.astype(jnp.bfloat16)
        if step == start:
            first_sent = rightward
        [from_left] = send([rightward], right_pairs(0, tp - step))
        [from_right] = send([leftward], left_pairs(step, tp))
    total = lax.optimization_barrier(part(me))
    if from_left is not None:
        total = total + from_left.astype(jnp.float32) + from_right.astype(jnp.float32)
    return total, first_sent


def body(x_tokens, segment_ids, attended_grad, norm_gain, w_query, w_key, w_value):
    head_dim = HD
    q_heads = w_query.shape[1] // head_dim
    kv_heads = w_key.shape[1] // head_dim
    segment_row = segment_ids[0]
    tp = lax.axis_size("tp")
    me = lax.axis_index("tp")
    rows = x_tokens.shape[0]
    seq_len = tp * rows
    query_cols = w_query.shape[1]
    key_cols = w_key.shape[1]
    relay = tp >= 4
    passed = end_weights(w_query, w_key, w_value, tp) if relay else None
    as_float = x_tokens.astype(jnp.float32)
    inverse = lax.rsqrt(jnp.mean(as_float * as_float, axis=1, keepdims=True) + epsilon)
    x_hat = as_float * inverse
    own = lax.optimization_barrier((x_hat * norm_gain).astype(jnp.bfloat16))
    own = list(lax.optimization_barrier(tuple(split_rows(own))))
    cosine_table, sine_table = rope_tables(segment_row, head_dim)
    weights = lax.optimization_barrier(jnp.concatenate([w_query, w_key, w_value], axis=1))

    def multiply(block, columns):
        return jnp.dot(block, columns, preferred_element_type=jnp.float32)

    def turn(product, place):
        cosine = lax.dynamic_slice_in_dim(cosine_table, place * rows, rows, 0)
        sine = lax.dynamic_slice_in_dim(sine_table, place * rows, rows, 0)
        turned = product[:, : query_cols + key_cols].reshape(rows, -1, head_dim)
        turned = apply_rope(turned, cosine, sine, 1.0).reshape(rows, -1)
        return jnp.concatenate(
            [turned.astype(jnp.bfloat16), product[:, query_cols + key_cols :].astype(jnp.bfloat16)],
            axis=1,
        )

    normed = jnp.zeros((seq_len, x_tokens.shape[1]), jnp.bfloat16)
    projected = jnp.zeros((seq_len, weights.shape[1]), jnp.bfloat16)
    found = line_gather(own, tp, me, tp - 1 if relay else tp)
    far_weights = None
    for index, (pieces, place) in enumerate(found):
        block = lax.optimization_barrier(jnp.concatenate(pieces, axis=0))
        normed = lax.dynamic_update_slice(normed, block, (place * rows, 0))
        source = block
        if relay and index == len(found) - 1:
            inward = [(1, 0), (tp - 2, tp - 1)]
            ready = turn(multiply(block, far_weights), place)
            ready, source = lax.optimization_barrier((ready, block))
            far_product = lax.ppermute(ready, "tp", inward)
        product = multiply(source, weights)
        if relay and index == 0:
            far_weights = shared(passed, product)
        product = turn(product, place)
        projected = lax.dynamic_update_slice(projected, product, (place * rows, 0))
    if relay:
        at_end = (me == 0) | (me == tp - 1)
        far_place = jnp.where(at_end, tp - 1 - me, me)
        kept = lax.dynamic_slice(projected, (far_place * rows, 0), (rows, projected.shape[1]))
        projected = lax.dynamic_update_slice(
            projected, jnp.where(at_end, far_product, kept), (far_place * rows, 0)
        )
        late, _ = lax.optimization_barrier((block, far_product))
        late = lax.ppermute(late, "tp", inward)
        kept = lax.dynamic_slice(normed, (far_place * rows, 0), (rows, normed.shape[1]))
        normed = lax.dynamic_update_slice(
            normed, jnp.where(at_end, late, kept), (far_place * rows, 0)
        )
    attended, query_d, key_d, value_flat = attend(
        projected, attended_grad, segment_row, cosine_table, sine_table, q_heads, kv_heads
    )
    columns_d = lax.optimization_barrier(
        jnp.concatenate([query_d, key_d, value_flat], axis=1)
    )
    normed_d, first_sent = line_scatter(columns_d, weights, far_weights, tp, me, rows)
    held_d, _ = lax.optimization_barrier((columns_d, first_sent))
    weights_d = lax.optimization_barrier(contract_first(normed, held_d).astype(jnp.bfloat16))
    merged = lax.psum_scatter(weights_d, "dp", scatter_dimension=0, tiled=True).astype(jnp.float32)
    gain_part = jnp.sum(weights.astype(jnp.float32) * weights_d.astype(jnp.float32), axis=1)
    gain_part = lax.optimization_barrier(gain_part / norm_gain)
    gain_grad = total_over(total_over(gain_part, "dp"), "tp")
    scaled_d = normed_d * norm_gain
    input_grad = (
        inverse * (scaled_d - x_hat * jnp.mean(scaled_d * x_hat, axis=1, keepdims=True))
    ).astype(jnp.bfloat16)
    grad_query = merged[:, :query_cols]
    grad_key = merged[:, query_cols : query_cols + key_cols]
    grad_value = merged[:, query_cols + key_cols :]
    return (attended, input_grad, gain_grad, grad_query, grad_key, grad_value)


def solution(mesh):
    placed = (
        P(("dp", "tp"), None),
        P("dp", None),
        P("dp", "tp"),
        P(),
        P(None, "tp"),
        P(None, "tp"),
        P(None, "tp"),
    )
    return jax.shard_map(
        body,
        mesh=mesh,
        in_specs=placed,
        out_specs=(
            P("dp", "tp"),
            P(("dp", "tp"), None),
            P(),
            P("dp", "tp"),
            P("dp", "tp"),
            P("dp", "tp"),
        ),
        check_vma=False,
    )
```

```python
import functools

import jax
import jax.numpy as jnp
from jax import lax
from jax.experimental import pallas as pl
from jax.experimental.pallas import tpu as pltpu
from jax.sharding import PartitionSpec as P


HD = 128


epsilon = 1e-05
rope_base = 500000.0


def rope_tables(segment_row, head_dim):
    length = segment_row.shape[0]
    earlier = (segment_row[None, :] < segment_row[:, None]).astype(jnp.int32)
    offset = jnp.arange(length, dtype=jnp.int32) - jnp.sum(earlier, axis=1)
    half_dim = head_dim // 2
    inverse_freq = rope_base ** (-(jnp.arange(half_dim, dtype=jnp.float32) * 2.0 / head_dim))
    angle = offset.astype(jnp.float32)[:, None] * inverse_freq[None, :]
    return (jnp.cos(angle)[:, None, :], jnp.sin(angle)[:, None, :])


def apply_rope(head_rows, cosine_table, sine_table, direction):
    half_dim = head_rows.shape[-1] // 2
    first_half = head_rows[..., :half_dim]
    second_half = head_rows[..., half_dim:]
    return jnp.concatenate(
        [
            first_half * cosine_table - direction * second_half * sine_table,
            second_half * cosine_table + direction * first_half * sine_table,
        ],
        axis=-1,
    )


def contract_first(left, right):
    return lax.dot_general(
        left, right, (((0,), (0,)), ((), ())), preferred_element_type=jnp.float32
    )


def contract_last(left, right):
    return lax.dot_general(
        left, right, (((1,), (1,)), ((), ())), preferred_element_type=jnp.float32
    )


def turn_back(rows_f, cosine, sine):
    return rows_f * cosine + pltpu.roll(rows_f, rows_f.shape[1] // 2, 1) * sine


def attention_kernel(
    block_rows, query_ref, key_ref, value_ref, grad_ref, segment_column, segment_line,
    cosine_ref, sine_ref, attended_ref, query_d_ref, key_d_ref, value_d_ref, key_sum, value_sum,
):
    member = pl.program_id(1)
    seq_len, head_dim = query_ref.shape
    score_scale = float(head_dim) ** (-0.5)

    @pl.when(member == 0)
    def _():
        key_sum[...] = jnp.zeros_like(key_sum)
        value_sum[...] = jnp.zeros_like(value_sum)

    for first in range(0, seq_len, block_rows):
        last = first + block_rows
        query = query_ref[first:last, :]
        grad = grad_ref[first:last, :]
        keys = key_ref[:last, :]
        values = value_ref[:last, :]
        scores = contract_last(query, keys) * score_scale
        row = lax.broadcasted_iota(jnp.int32, scores.shape, 0) + first
        column = lax.broadcasted_iota(jnp.int32, scores.shape, 1)
        same = segment_column[first:last, :] == segment_line[:, :last]
        scores = jnp.where((column <= row) & same, scores, -1e30)
        exponent = jnp.exp(scores - jnp.max(scores, axis=1, keepdims=True))
        probability = exponent * (1.0 / jnp.sum(exponent, axis=1, keepdims=True))
        weights_b = probability.astype(jnp.bfloat16)
        attended = jnp.dot(weights_b, values, preferred_element_type=jnp.float32)
        attended = attended.astype(jnp.bfloat16)
        attended_ref[first:last, :] = attended
        row_delta = jnp.sum(
            grad.astype(jnp.float32) * attended.astype(jnp.float32), axis=1, keepdims=True
        )
        value_sum[:last, :] += contract_first(weights_b, grad)
        prob_d = contract_last(grad, values)
        score_d = (probability * (prob_d - row_delta) * score_scale).astype(jnp.bfloat16)
        query_rot = jnp.dot(score_d, keys, preferred_element_type=jnp.float32)
        query_d_ref[first:last, :] = turn_back(
            query_rot, cosine_ref[first:last, :], sine_ref[first:last, :]
        ).astype(jnp.bfloat16)
        key_sum[:last, :] += contract_first(score_d, query)

    @pl.when(member == pl.num_programs(1) - 1)
    def _():
        key_d_ref[...] = turn_back(key_sum[...], cosine_ref[...], sine_ref[...]).astype(
            jnp.bfloat16
        )
        value_d_ref[...] = value_sum[...].astype(jnp.bfloat16)


def attend(projected, attended_grad, segment_row, cosine_table, sine_table, q_heads, kv_heads):
    seq_len, head_dim = projected.shape[0], HD
    group = q_heads // kv_heads
    block_rows = 256 if seq_len % 256 == 0 else seq_len
    cosine = jnp.concatenate([cosine_table[:, 0], cosine_table[:, 0]], axis=1)
    sine = jnp.concatenate([sine_table[:, 0], -sine_table[:, 0]], axis=1)

    def head(index_of):
        return pl.BlockSpec((seq_len, head_dim), lambda k, m: (0, index_of(k, m)))

    def whole(shape):
        return pl.BlockSpec(shape, lambda k, m: (0, 0))

    of_query = head(lambda k, m: k * group + m)
    of_key = head(lambda k, m: k)
    pairs = q_heads * seq_len * seq_len
    return pl.pallas_call(
        functools.partial(attention_kernel, block_rows),
        grid=(kv_heads, group),
        in_specs=[
            of_query,
            head(lambda k, m: q_heads + k),
            head(lambda k, m: q_heads + kv_heads + k),
            of_query,
            whole((seq_len, 1)),
            whole((1, seq_len)),
            whole((seq_len, head_dim)),
            whole((seq_len, head_dim)),
        ],
        out_specs=[of_query, of_query, of_key, of_key],
        out_shape=[
            jax.ShapeDtypeStruct((seq_len, heads * head_dim), jnp.bfloat16)
            for heads in (q_heads, q_heads, kv_heads, kv_heads)
        ],
        scratch_shapes=[pltpu.VMEM((seq_len, head_dim), jnp.float32)] * 2,
        cost_estimate=pl.CostEstimate(
            flops=8 * pairs * head_dim, bytes_accessed=10 * projected.size, transcendentals=pairs
        ),
    )(
        projected, projected, projected, attended_grad, segment_row[:, None],
        segment_row[None, :], cosine, sine,
    )


def total_over(value, axis):
    size = lax.axis_size(axis)
    if size & (size - 1):
        return lax.psum(value, axis)
    apart = 1
    while apart < size:
        value = value + lax.ppermute(value, axis, [(i, i ^ apart) for i in range(size)])
        apart *= 2
    return value


def right_pairs(low, high):
    return [(i, i + 1) for i in range(low, high)]


def left_pairs(low, high):
    return [(i, i - 1) for i in range(low, high)]


def split_rows(block):
    half = block.shape[0] // 2
    return [block[:half], block[half:]]


def send(pieces, pairs):
    sent = []
    for piece in pieces:
        sent.append(lax.ppermute(piece, "tp", pairs))
    return sent


def end_weights(w_query, w_key, w_value, tp):
    share = w_query.shape[0] // lax.axis_size("dp")
    first = lax.axis_index("dp") * share
    cut = [lax.dynamic_slice_in_dim(w, first, share, 0) for w in (w_query, w_key, w_value)]
    cut = lax.optimization_barrier(jnp.concatenate(cut, axis=1))
    [passed] = send([cut], [(0, 1), (tp - 1, tp - 2)])
    return passed


def shared(passed, after):
    passed, _ = lax.optimization_barrier((passed, after))
    return lax.all_gather(passed, "dp", axis=0, tiled=True)


def line_gather(own, tp, me, steps):
    found = [[(own, me)]]
    rightward = leftward = own
    for step in range(1, steps):
        rightward = send(rightward, right_pairs(step - 1, tp - 1))
        leftward = send(leftward, left_pairs(1, tp - step + 1))
        if 2 * step >= tp:
            left_over = leftward
            place = jnp.where(me >= step, me - step, me + step)
            if 2 * step > tp:
                empty = (me < step) & (me + step >= tp)
                left_over = [jnp.where(empty, o, l) for o, l in zip(own, leftward)]
                place = jnp.where(empty, me, place)
            chosen = [jnp.where(me >= step, r, l) for r, l in zip(rightward, left_over)]
            found.append([(chosen, place)])
        else:
            before, after = (me - step + tp) % tp, (me + step) % tp
            found.append([(rightward, before), (leftward, after)])
    return found


def line_scatter(columns_d, weights, far_weights, tp, me, rows, between):
    features = weights.shape[0]
    halves = ((0, features // 2), (features // 2, features))

    def rows_of(place):
        return lax.dynamic_slice(columns_d, (place * rows, 0), (rows, columns_d.shape[1]))

    def part(place):
        return lax.optimization_barrier(contract_last(rows_of(place), weights))

    def ahead_of(step):
        return jnp.where(me + step < tp, me + step, (me - step + tp) % tp)

    def plus(sums, index, received):
        low, high = halves[index]
        sums = sums[:, low:high]
        for item in received:
            sums = sums + item.astype(jnp.float32)
        return sums

    far = None
    start = tp - 1
    if far_weights is not None:
        far = lax.optimization_barrier(rows_of(tp - 1 - me))
        far = lax.ppermute(far, "tp", [(0, 1), (tp - 1, tp - 2)])
        start = tp - 2
    result = None
    received = [(), ()]
    for step in range(start, 0, -1):
        joint = 2 * step >= tp
        if joint:
            right_part = left_part = part(ahead_of(step))
        else:
            both = [rows_of((me + step) % tp), rows_of((me - step + tp) % tp)]
            both = contract_last(jnp.concatenate(both, axis=0), weights)
            both = lax.optimization_barrier(both)
            right_part, left_part = both[:rows], both[rows:]
        sent = []
        for index, (low, high) in enumerate(halves):
            got = received[index]
            if step == start and far is not None:
                got = (contract_last(far, far_weights[low:high]),)
            if joint:
                rightward = leftward = lax.optimization_barrier(
                    plus(right_part, index, got).astype(jnp.bfloat16)
                )
            else:
                rightward = plus(right_part, index, got[:1]).astype(jnp.bfloat16)
                leftward = plus(left_part, index, got[1:]).astype(jnp.bfloat16)
                both, rightward, leftward = lax.optimization_barrier((both, rightward, leftward))
                right_part, left_part = both[:rows], both[rows:]
            [from_left] = send([rightward], right_pairs(0, tp - step))
            [from_right] = send([leftward], left_pairs(step, tp))
            sent.append((from_left, from_right))
            if result is None:
                result = between(rightward)
                if far is not None:
                    far, _ = lax.optimization_barrier((far, result))
        received = sent
    if result is None:
        result = between(columns_d)
    total = part(me)
    total = [plus(total, index, received[index]) for index in range(2)]
    return jnp.concatenate(total, axis=1), result


def body(x_tokens, segment_ids, attended_grad, norm_gain, w_query, w_key, w_value):
    head_dim = HD
    q_heads = w_query.shape[1] // head_dim
    kv_heads = w_key.shape[1] // head_dim
    segment_row = segment_ids[0]
    tp = lax.axis_size("tp")
    me = lax.axis_index("tp")
    rows = x_tokens.shape[0]
    seq_len = tp * rows
    query_cols = w_query.shape[1]
    key_cols = w_key.shape[1]
    relay = tp >= 4
    passed = end_weights(w_query, w_key, w_value, tp) if relay else None
    as_float = x_tokens.astype(jnp.float32)
    inverse = lax.rsqrt(jnp.mean(as_float * as_float, axis=1, keepdims=True) + epsilon)
    x_hat = as_float * inverse
    own = lax.optimization_barrier((x_hat * norm_gain).astype(jnp.bfloat16))
    own = list(lax.optimization_barrier(tuple(split_rows(own))))
    cosine_table, sine_table = rope_tables(segment_row, head_dim)
    weights = lax.optimization_barrier(jnp.concatenate([w_query, w_key, w_value], axis=1))

    def multiply(block, columns):
        return jnp.dot(block, columns, preferred_element_type=jnp.float32)

    def turn(product, place):
        cosine = lax.dynamic_slice_in_dim(cosine_table, place * rows, rows, 0)
        sine = lax.dynamic_slice_in_dim(sine_table, place * rows, rows, 0)
        turned = product[:, : query_cols + key_cols].reshape(rows, -1, head_dim)
        turned = apply_rope(turned, cosine, sine, 1.0).reshape(rows, -1)
        return jnp.concatenate(
            [turned.astype(jnp.bfloat16), product[:, query_cols + key_cols :].astype(jnp.bfloat16)],
            axis=1,
        )

    normed = jnp.zeros((seq_len, x_tokens.shape[1]), jnp.bfloat16)
    projected = jnp.zeros((seq_len, weights.shape[1]), jnp.bfloat16)
    found = line_gather(own, tp, me, tp - 1 if relay else tp)
    far_weights = None
    for index, batch in enumerate(found):
        block = jnp.concatenate([piece for pieces, _ in batch for piece in pieces], axis=0)
        block = lax.optimization_barrier(block)
        source = block
        if relay and index == len(found) - 1:
            inward = [(1, 0), (tp - 2, tp - 1)]
            ready = turn(multiply(block, far_weights), batch[0][1])
            ready, source = lax.optimization_barrier((ready, block))
            far_product = lax.ppermute(ready, "tp", inward)
        product = multiply(source, weights)
        if relay and index == 0:
            far_weights = shared(passed, product)
        for number, (_, place) in enumerate(batch):
            mine = slice(number * rows, (number + 1) * rows)
            normed = lax.dynamic_update_slice(normed, block[mine], (place * rows, 0))
            turned = turn(product[mine], place)
            projected = lax.dynamic_update_slice(projected, turned, (place * rows, 0))
    if relay:
        at_end = (me == 0) | (me == tp - 1)
        far_place = jnp.where(at_end, tp - 1 - me, me)
        kept = lax.dynamic_slice(projected, (far_place * rows, 0), (rows, projected.shape[1]))
        projected = lax.dynamic_update_slice(
            projected, jnp.where(at_end, far_product, kept), (far_place * rows, 0)
        )
        early = rows // 4
        late, _ = lax.optimization_barrier((block[early:], far_product))
        late = send([lax.optimization_barrier(block[:early])], inward) + send([late], inward)
        late = jnp.concatenate(late, axis=0)
        kept = lax.dynamic_slice(normed, (far_place * rows, 0), (rows, normed.shape[1]))
        normed = lax.dynamic_update_slice(
            normed, jnp.where(at_end, late, kept), (far_place * rows, 0)
        )
    attended, query_d, key_d, value_flat = attend(
        projected, attended_grad, segment_row, cosine_table, sine_table, q_heads, kv_heads
    )
    columns_d = lax.optimization_barrier(
        jnp.concatenate([query_d, key_d, value_flat], axis=1)
    )

    def weights_grad(after):
        held_d, _ = lax.optimization_barrier((columns_d, after))
        return lax.optimization_barrier(contract_first(normed, held_d).astype(jnp.bfloat16))

    normed_d, weights_d = line_scatter(
        columns_d, weights, far_weights, tp, me, rows, weights_grad
    )
    merged = lax.psum_scatter(weights_d, "dp", scatter_dimension=0, tiled=True).astype(jnp.float32)
    gain_part = jnp.sum(weights.astype(jnp.float32) * weights_d.astype(jnp.float32), axis=1)
    gain_part = lax.optimization_barrier(gain_part / norm_gain)
    gain_grad = total_over(total_over(gain_part, "dp"), "tp")
    scaled_d = normed_d * norm_gain
    input_grad = (
        inverse * (scaled_d - x_hat * jnp.mean(scaled_d * x_hat, axis=1, keepdims=True))
    ).astype(jnp.bfloat16)
    grad_query = merged[:, :query_cols]
    grad_key = merged[:, query_cols : query_cols + key_cols]
    grad_value = merged[:, query_cols + key_cols :]
    return (attended, input_grad, gain_grad, grad_query, grad_key, grad_value)


def solution(mesh):
    placed = (
        P(("dp", "tp"), None),
        P("dp", None),
        P("dp", "tp"),
        P(),
        P(None, "tp"),
        P(None, "tp"),
        P(None, "tp"),
    )
    return jax.shard_map(
        body,
        mesh=mesh,
        in_specs=placed,
        out_specs=(
            P("dp", "tp"),
            P(("dp", "tp"), None),
            P(),
            P("dp", "tp"),
            P("dp", "tp"),
            P("dp", "tp"),
        ),
        check_vma=False,
    )
```
